1024 devices in a mesh: dp: 128 (over z, x, core), slab: 8 (over y).
Axes of the slice: x: 4, y: 8, z: 16, core: 2. Of those that a mesh axis runs over, the one named last changes fastest.
Arguments:
- inputs: bfloat16 [128, 48, 34944], P('dp', 'slab'), may hold values from -40 to 40
- upstream: bfloat16 [128, 48, 34944], P('dp', 'slab'), may hold values from -96 to 96
- labels: int32 [128, 48, 48], P('dp', 'slab'), may hold values from 0 to 2
- class_weights: float32 [3], replicated, may hold values from 0.25 to 4
- depth_kernel: bfloat16 [9, 728], replicated, may hold values from -2 to 2
- point_weight: bfloat16 [728, 728], replicated, may hold values from -0.21875 to 0.21875
- gain: float32 [728], replicated, may hold values from 0.5 to 1.5
- shift: float32 [728], replicated, may hold values from -3 to 3
Outputs:
- block_out: bfloat16 [128, 48, 34944], P('dp', 'slab')
- grad_input: bfloat16 [128, 48, 34944], P('dp', 'slab')
- grad_pointwise: float32 [728, 728], P(None, 'slab')
- grad_depthwise: float32 [9, 728], P(None, 'slab')
- grad_gain: float32 [728], P('slab')
- grad_shift: float32 [728], P('slab')
The draws below stay inside these ranges and needn't reach their ends.
All inputs are finite; a program needn't handle non-finite values.
Results may differ from the reference program's by a relative error of at most 0.0052.
The reference program's roundings to bfloat16 on the way (of `active`, `depth`, `grad_proj` and `grad_depth`) count: a program that leaves them out, or rounds other values in their place, can miss the bound.
Values may be sent and summed in bfloat16 or wider, within the bound.
A program may use at most 32 MiB of HBM per device.

```python
import math
import jax
import jax.numpy as jnp
from jax import lax

CH = 728
WIDTH = 48
SAMP_DEV = 1
BATCH = 128
HEIGHT = 48
N_DP = 128


def rise_profile():
    return 3.0 ** (jnp.arange(HEIGHT, dtype=jnp.float32) / max(HEIGHT - 1, 1))


def draw_inputs(key, part):
    first = jax.random.fold_in(jax.random.fold_in(key, 11), 0)
    third = jax.random.fold_in(jax.random.fold_in(key, 11), 2)
    base = jax.random.normal(first, (BATCH, HEIGHT, WIDTH, CH), jnp.float32)
    rough = jnp.exp(jax.random.uniform(third, (BATCH, HEIGHT, WIDTH, 1), jnp.float32, -0.5 * math.log(2.0), 0.5 * math.log(2.0)))
    values = jnp.clip(base * rough * rise_profile()[None, :, None, None], -40.0, 40.0)
    return values.reshape(BATCH, HEIGHT, WIDTH * CH).astype(jnp.bfloat16)


def draw_upstream(key, part):
    first = jax.random.fold_in(jax.random.fold_in(key, 23), 0)
    third = jax.random.fold_in(jax.random.fold_in(key, 23), 2)
    fourth = jax.random.fold_in(key, 37)
    base = jax.random.normal(first, (BATCH, HEIGHT, WIDTH, CH), jnp.float32)
    rough = jnp.exp(jax.random.uniform(third, (BATCH, HEIGHT, WIDTH, 1), jnp.float32, -0.5 * math.log(2.0), 0.5 * math.log(2.0)))
    partner = jax.random.permutation(fourth, BATCH)
    channel_slot = jnp.arange(CH, dtype=jnp.int32) % BATCH
    heavy = jnp.where(channel_slot[None, :] == partner[:, None], 8.0, 1.0).astype(jnp.float32)
    values = base * rough * rise_profile()[None, :, None, None] * heavy[:, None, None, :]
    values = jnp.clip(values, -96.0, 96.0)
    return values.reshape(BATCH, HEIGHT, WIDTH * CH).astype(jnp.bfloat16)


def plant(entries, rng, low, largest):
    longest = entries.shape.index(max(entries.shape))
    spots = []
    for shift in (0, 1):
        where = [jax.random.randint(jax.random.fold_in(rng, axis), (), 0, length) for axis, length in enumerate(entries.shape)]
        where[longest] = (where[longest] + shift) % entries.shape[longest]
        spots.append(tuple(where))
    return entries.at[spots[0]].set(low).at[spots[1]].set(largest)


def normal_values(key, extent, scale, most, kind=jnp.bfloat16):
    return jnp.clip(scale * jax.random.normal(key, extent, jnp.float32), -most, most).astype(kind)


def setup_inputs(seed: int = 0) -> dict:
    splits = jax.random.split(jax.random.key(seed), 9)
    inputs = draw_inputs(jax.random.fold_in(splits[8], 71), 0)
    upstream = draw_upstream(jax.random.fold_in(splits[8], 71), 0)
    labels = plant(jax.random.randint(splits[2], (BATCH, HEIGHT, WIDTH), 0, 3), jax.random.fold_in(splits[2], 1), 0, 2).astype(jnp.int32)
    class_weights = jnp.clip(jnp.exp(jax.random.uniform(splits[3], (3,), jnp.float32, math.log(0.25), math.log(4.0))), 0.25, 4.0)
    depth_kernel = normal_values(splits[4], (9, CH), 9 ** -0.5, 2.0)
    point_weight = normal_values(splits[5], (CH, CH), CH ** -0.5, 0.21875)
    gain = jnp.clip(1.0 + 0.1 * jax.random.normal(splits[6], (CH,), jnp.float32), 0.5, 1.5)
    shift = normal_values(splits[7], (CH,), 0.5, 3.0, jnp.float32)
    return dict(inputs=inputs, upstream=upstream, labels=labels, class_weights=class_weights, depth_kernel=depth_kernel, point_weight=point_weight, gain=gain, shift=shift)


def widen_columns(values):
    return jnp.pad(values, ((0, 0), (0, 0), (1, 1), (0, 0)))

def depthwise(padded, kernel):
    row_count = padded.shape[1] - 2
    col_count = padded.shape[2]
    widened = widen_columns(padded)
    summed = jnp.zeros((padded.shape[0], row_count, col_count, padded.shape[3]), jnp.float32)
    for row_tap in range(3):
        for col_tap in range(3):
            window = widened[:, row_tap:row_tap + row_count, col_tap:col_tap + col_count, :]
            summed = summed + window.astype(jnp.float32) * kernel[3 * row_tap + col_tap].astype(jnp.float32)
    return summed

def transposed(padded_grad, kernel):
    row_count = padded_grad.shape[1] - 2
    col_count = padded_grad.shape[2]
    widened = widen_columns(padded_grad)
    summed = jnp.zeros((padded_grad.shape[0], row_count, col_count, padded_grad.shape[3]), jnp.float32)
    for row_tap in range(3):
        for col_tap in range(3):
            window = widened[:, 2 - row_tap:2 - row_tap + row_count, 2 - col_tap:2 - col_tap + col_count, :]
            summed = summed + window.astype(jnp.float32) * kernel[3 * row_tap + col_tap].astype(jnp.float32)
    return summed

def taps(padded, grad_image):
    row_count = grad_image.shape[1]
    col_count = grad_image.shape[2]
    widened = widen_columns(padded)
    results = []
    for row_tap in range(3):
        for col_tap in range(3):
            window = widened[:, row_tap:row_tap + row_count, col_tap:col_tap + col_count, :]
            results.append(jnp.einsum('srwc,srwc->c', window.astype(jnp.float32), grad_image.astype(jnp.float32), precision=lax.Precision.HIGHEST))
    return jnp.stack(results)

def reference(inputs, upstream, labels, class_weights, depth_kernel, point_weight, gain, shift):
    image = inputs.reshape(N_DP, SAMP_DEV, HEIGHT, WIDTH, CH)
    cotangent = upstream.reshape(N_DP, SAMP_DEV, HEIGHT, WIDTH, CH)
    classes = labels.reshape(N_DP, SAMP_DEV * HEIGHT * WIDTH)

    def group_step(running, group_items):
        sample, incoming, label_group = group_items
        active = jnp.maximum(sample, 0)
        padded = jnp.pad(active, ((0, 0), (1, 1), (0, 0), (0, 0)))
        depth = depthwise(padded, depth_kernel).astype(jnp.bfloat16)
        flat_depth = depth.reshape(-1, CH)
        projected = jnp.dot(flat_depth, point_weight, preferred_element_type=jnp.float32)
        center = lax.optimization_barrier(jnp.mean(projected, axis=0))
        spread = lax.optimization_barrier(jnp.mean((projected - center) ** 2, axis=0))
        inverse = lax.rsqrt(spread + 1e-05)
        normed = (projected - center) * inverse
        result = sample.reshape(-1, CH).astype(jnp.float32) + gain * normed + shift
        match = label_group[:, None] == jnp.arange(3, dtype=jnp.int32)[None, :]
        weight = lax.optimization_barrier(jnp.sum(jnp.where(match, class_weights[None, :], 0.0), axis=1))
        grad_out = incoming.reshape(-1, CH).astype(jnp.float32) * weight[:, None]
        count = projected.shape[0]
        shift_part = lax.optimization_barrier(jnp.sum(grad_out, axis=0))
        gain_part = lax.optimization_barrier(jnp.sum(grad_out * normed, axis=0))
        grad_proj = (gain * inverse * (grad_out - shift_part / count - normed * gain_part / count)).astype(jnp.bfloat16)
        grad_depth = jnp.dot(grad_proj, point_weight.T, preferred_element_type=jnp.float32).astype(jnp.bfloat16)
        point_part = jnp.dot(flat_depth.T, grad_proj, preferred_element_type=jnp.float32)
        grad_image = grad_depth.reshape(depth.shape)
        padded_grad = jnp.pad(grad_image, ((0, 0), (1, 1), (0, 0), (0, 0)))
        grad_active = transposed(padded_grad, depth_kernel).reshape(-1, CH)
        grad_input = grad_out + jnp.where(sample.reshape(-1, CH) > 0, grad_active, 0.0)
        tap_part = taps(padded, grad_image)
        running = (running[0] + point_part, running[1] + tap_part, running[2] + gain_part, running[3] + shift_part)
        return (running, (result.astype(jnp.bfloat16), grad_input.astype(jnp.bfloat16)))
    start = (jnp.zeros((CH, CH), jnp.float32), jnp.zeros((9, CH), jnp.float32), jnp.zeros((CH,), jnp.float32), jnp.zeros((CH,), jnp.float32))
    totals, outputs = lax.scan(group_step, start, (image, cotangent, classes))
    block_out = outputs[0].reshape(BATCH, HEIGHT, WIDTH * CH)
    grad_input = outputs[1].reshape(BATCH, HEIGHT, WIDTH * CH)
    return (block_out, grad_input, totals[0] / BATCH, totals[1] / BATCH, totals[2] / BATCH, totals[3] / BATCH)
```

```python
import functools

import jax
import jax.numpy as jnp
from jax import lax
from jax.experimental import pallas as pl
from jax.experimental.pallas import tpu as pltpu
from jax.sharding import PartitionSpec as P

MESH = pl.DeviceIdType.MESH
F32 = jnp.float32
BF16 = jnp.bfloat16

CH = 728
CP = 768
CB = CP // 128
WIDTH = 48
ROWS = 6
PIX = WIDTH * 8
GROUP = 16 * CH // 128
NZ, NX, NC, NY = 16, 4, 2, 8
SHARE = CH // NY
HALF = 48
NH = NY * HALF
TILES = HALF // 8 * CB
TX = TILES // NX
RED = [NZ * i // TX for i in range(TX)]
COUNT = float(ROWS * WIDTH * NY)
BATCH = float(NZ * NX * NC)


def lanes(i):
    return slice(128 * i, 128 * (i + 1))


def kernel(
    x_ref, u_ref, lab_ref, cw_ref, dk_ref, pw_ref, gain_ref, shift_ref,
    out_ref, gin_ref, gpw_ref, gdw_ref, gg_ref, gs_ref,
    X, A, U, PJ, D, GP, GD, WP, ST, SEL, RR, RS, GS, GR, H, RF, RB, VX, VZ, C, CM,
    HS, HR, BS, BR, STAT, VEC, RRECV,
    h_send, h_recv, b_send, b_recv, s_send, s_recv, g_send, g_recv,
    f_send, f_recv, k_send, k_recv, x_send, x_recv, z_send, z_recv,
    a_send, a_recv, ax_send, ax_recv, ac_send, ac_recv,
):
    dp = lax.axis_index("dp")
    y = lax.axis_index("slab")
    c = lax.rem(dp, NC)
    xx = lax.rem(dp // NC, NX)
    z = dp // (NC * NX)

    def at_y(k):
        return (dp, lax.rem(y + (k % NY), NY))

    def at_x(k):
        return ((z * NX + lax.rem(xx + (k % NX), NX)) * NC + c, y)

    def at_zz(zz):
        return ((zz * NX + xx) * NC + c, y)

    partner = ((z * NX + xx) * NC + (1 - c), y)

    def rcopy(src, dst, ss, rs, dev):
        return pltpu.make_async_remote_copy(
            src_ref=src, dst_ref=dst, send_sem=ss, recv_sem=rs,
            device_id=dev, device_id_type=MESH,
        )

    barrier = pltpu.get_barrier_semaphore()
    peers = [at_y(k) for k in range(1, NY)]
    peers += [at_x(k) for k in range(1, NX)]
    peers += [at_zz(lax.rem(z + k, NZ)) for k in range(1, NZ)]
    peers += [partner]
    for peer in peers:
        pl.semaphore_signal(barrier, inc=1, device_id=peer, device_id_type=MESH)

    lane_ok = lax.broadcasted_iota(jnp.int32, (ROWS, CP), 1) < CH

    def unflat(ref, base, k):
        off = CH * k
        first, sh = off // 128, off % 128
        nv = 6 if sh + CH <= CP else 7
        v = ref[:, pl.ds(pl.multiple_of(base + first * 128, 128), nv * 128)].astype(F32)
        if sh:
            v = pltpu.roll(v, nv * 128 - sh, axis=1)
        return jnp.where(lane_ok, v[:, :CP], 0.0)

    X[...] = jnp.zeros_like(X)

    def load_x(g, carry):
        for k in range(16):
            X[g * 16 + k, 0:ROWS, :] = unflat(x_ref, g * GROUP * 128, k)
        return carry

    lax.fori_loop(0, WIDTH // 16, load_x, 0)
    for side, row in ((0, 0), (1, ROWS - 1)):
        HS[side] = X[:, row, :].astype(BF16)

    lab = lab_ref[...]
    wt = jnp.where(
        lab == 0, cw_ref[0], jnp.where(lab == 1, cw_ref[1], jnp.where(lab == 2, cw_ref[2], 0.0))
    )
    U[...] = jnp.zeros_like(U)
    for w in range(WIDTH):
        U[w, 0:ROWS, :] = unflat(u_ref, (w // 16) * GROUP * 128, w % 16) * wt[:, w : w + 1]

    pl.semaphore_wait(barrier, len(peers))

    halo = [
        rcopy(HS.at[0], HR.at[0], h_send.at[0], h_recv.at[0], at_y(-1)),
        rcopy(HS.at[1], HR.at[1], h_send.at[1], h_recv.at[1], at_y(1)),
    ]
    for cp in halo:
        cp.start()

    WP[...] = jnp.zeros_like(WP)
    WP[0:CH, 0:CH] = pw_ref[...]
    row = lax.broadcasted_iota(jnp.int32, (NH, 128), 0)
    slab_of = jnp.zeros_like(row)
    for k in range(1, NY):
        slab_of = slab_of + jnp.where(row >= HALF * k, 1, 0)
    inner = row - HALF * slab_of
    lane = lax.broadcasted_iota(jnp.int32, (NH, 128), 1)
    for h in range(2):
        core = (1 - c) if h == 0 else c
        j = inner + HALF * core
        target = jnp.where(j < SHARE, SHARE * slab_of + j, -1)
        for b in range(CB):
            ST[h, :, lanes(b)] = jnp.where(lane + 128 * b == target, 1.0, 0.0).astype(BF16)

    for cp in halo:
        cp.wait()
    below = jnp.where(y < NY - 1, HR[0].astype(F32), 0.0)
    above = jnp.where(y > 0, HR[1].astype(F32), 0.0)
    X[:, ROWS, :] = below
    X[:, ROWS + 1, :] = above
    A[0] = jnp.zeros((8, CP), F32)
    A[WIDTH + 1] = jnp.zeros((8, CP), F32)
    A[1 : WIDTH + 1] = jnp.maximum(X[...], 0.0)

    own = lax.broadcasted_iota(jnp.int32, (8, 8, 128), 1) < ROWS
    own2 = lax.broadcasted_iota(jnp.int32, (8, 8, 128), 1) < ROWS

    for b in range(CB):
        k = [dk_ref[t : t + 1, lanes(b)].astype(F32) for t in range(9)]

        def conv(q, carry):
            a = A[pl.ds(q * 8, 10), :, lanes(b)]
            rows = [
                a[0:8] * k[3 * i] + a[1:9] * k[3 * i + 1] + a[2:10] * k[3 * i + 2]
                for i in range(3)
            ]
            d = pltpu.roll(rows[0], 1, axis=1) + rows[1] + pltpu.roll(rows[2], 7, axis=1)
            d = jnp.where(own, d, 0.0)
            D[pl.ds(pl.multiple_of(q * 64, 64), 64), lanes(b)] = d.reshape(64, 128).astype(BF16)
            return carry

        lax.fori_loop(0, WIDTH // 8, conv, 0)

    for nb in range(3):
        cols = slice(256 * nb, 256 * (nb + 1))
        PJ[:, :, cols] = jnp.dot(
            D[...], WP[:, cols], preferred_element_type=F32
        ).reshape(WIDTH, 8, 256)

    n_local = float(ROWS * WIDTH)
    for b in range(CB):
        s = jnp.zeros((8, 128), F32)
        g = jnp.zeros((8, 128), F32)
        for q in range(WIDTH // 8):
            s = s + jnp.sum(PJ[8 * q : 8 * q + 8, :, lanes(b)], axis=0)
            g = g + jnp.sum(U[8 * q : 8 * q + 8, :, lanes(b)], axis=0)
        s = jnp.sum(s, axis=0, keepdims=True)
        g = jnp.sum(g, axis=0, keepdims=True)
        mu = s * (1.0 / n_local)
        m2 = jnp.zeros((8, 128), F32)
        cr = jnp.zeros((8, 128), F32)
        for q in range(WIDTH // 8):
            dev = jnp.where(own2, PJ[8 * q : 8 * q + 8, :, lanes(b)] - mu, 0.0)
            m2 = m2 + jnp.sum(dev * dev, axis=0)
            cr = cr + jnp.sum(dev * U[8 * q : 8 * q + 8, :, lanes(b)], axis=0)
        m2 = jnp.sum(m2, axis=0, keepdims=True)
        cr = jnp.sum(cr, axis=0, keepdims=True)
        STAT[y, :, lanes(b)] = jnp.concatenate([s, g, m2, cr], axis=0)
    stat = []
    for k in range(1, NY):
        cp = rcopy(STAT.at[y], STAT.at[y], s_send.at[k - 1], s_recv.at[k - 1], at_y(k))
        cp.start()
        stat.append(cp)
    for cp in stat:
        cp.wait()

    total = STAT[0, 0:2, :]
    for i in range(1, NY):
        total = total + STAT[i, 0:2, :]
    center = total[0:1] * (1.0 / COUNT)
    shift_part = total[1:2]
    square = jnp.zeros((1, CP), F32)
    cross = jnp.zeros((1, CP), F32)
    for i in range(NY):
        off = STAT[i, 0:1, :] * (1.0 / n_local) - center
        square = square + STAT[i, 2:3, :] + n_local * off * off
        cross = cross + STAT[i, 3:4, :] + off * STAT[i, 1:2, :]
    inverse = lax.rsqrt(square * (1.0 / COUNT) + 1e-05)
    gain_part = cross * inverse
    mine = STAT[y]
    off = mine[0:1] * (1.0 / n_local) - center
    gain_local = (mine[3:4] + off * mine[1:2]) * inverse
    shift_local = mine[1:2]
    gain = gain_ref[...]
    VEC[0:1] = center
    VEC[1:2] = inverse
    VEC[2:3] = gain
    VEC[3:4] = shift_ref[...]
    VEC[4:5] = gain * inverse
    VEC[5:6] = shift_part * (1.0 / COUNT)
    VEC[6:7] = gain_part * (1.0 / COUNT)

    for b in range(CB):
        v = [VEC[i : i + 1, lanes(b)] for i in range(7)]

        def proj(q, carry):
            rows = pl.ds(q * 8, 8)
            normed = (PJ[rows, :, lanes(b)] - v[0]) * v[1]
            gp = v[4] * (U[rows, :, lanes(b)] - v[5] - normed * v[6])
            gp = jnp.where(own, gp, 0.0)
            GP[pl.ds(pl.multiple_of(q * 64, 64), 64), lanes(b)] = gp.reshape(64, 128).astype(BF16)
            return carry

        lax.fori_loop(0, WIDTH // 8, proj, 0)

    NT = (((1,), (1,)), ((), ()))

    def weight_half(h, dst):
        SEL[...] = lax.dot_general(
            ST[h], GP[...], NT, preferred_element_type=F32
        ).astype(BF16)
        for nb in range(3):
            part = jnp.dot(
                SEL[...], D[:, 256 * nb : 256 * nb + 256], preferred_element_type=F32
            )
            for s in range(NY):
                for i in range(HALF // 8):
                    for j in range(2):
                        r = HALF * s + 8 * i
                        dst[s, i * CB + 2 * nb + j] = part[r : r + 8, lanes(j)]

    weight_half(0, GS)
    g_copy = rcopy(GS, GR, g_send.at[0], g_recv.at[0], partner)
    g_copy.start()

    GD[0] = jnp.zeros((8, CP), F32)
    GD[WIDTH + 1] = jnp.zeros((8, CP), F32)
    for nb in range(3):
        rows = slice(256 * nb, 256 * (nb + 1))
        gd = lax.dot_general(GP[...], WP[rows, :], NT, preferred_element_type=F32)
        GD[1 : WIDTH + 1, :, rows] = gd.astype(BF16).astype(F32).reshape(WIDTH, 8, 256)
    BS[0] = GD[1 : WIDTH + 1, 0, :].astype(BF16)
    BS[1] = GD[1 : WIDTH + 1, ROWS - 1, :].astype(BF16)
    back = [
        rcopy(BS.at[0], BR.at[0], b_send.at[0], b_recv.at[0], at_y(-1)),
        rcopy(BS.at[1], BR.at[1], b_send.at[1], b_recv.at[1], at_y(1)),
    ]
    for cp in back:
        cp.start()

    RR[...] = jnp.zeros_like(RR)
    for b in range(CB):

        def tap(q, acc):
            a = A[pl.ds(q * 8, 10), :, lanes(b)]
            gd = GD[pl.ds(q * 8 + 1, 8), :, lanes(b)]
            shifted = [pltpu.roll(gd, 7, axis=1), gd, pltpu.roll(gd, 1, axis=1)]
            return tuple(
                acc[3 * i + j] + jnp.sum(a[j : j + 8] * shifted[i], axis=0)
                for i in range(3)
                for j in range(3)
            )

        acc = lax.fori_loop(
            0, WIDTH // 8, tap, tuple(jnp.zeros((8, 128), F32) for _ in range(9))
        )
        for t in range(9):
            RR[t : t + 1, lanes(b)] = jnp.sum(acc[t], axis=0, keepdims=True)
    RR[9:10] = gain_local
    RR[10:11] = shift_local
    r_copy = rcopy(RR, RRECV, g_send.at[1], g_recv.at[1], partner)
    r_copy.start()

    weight_half(1, H)
    RS[...] = jnp.zeros_like(RS)
    g_copy.wait()
    r_copy.wait()
    RS[CH - 640 : CH - 640 + 16] = RR[...] + RRECV[...]
    rest = RS[...]
    extra = jnp.zeros((NH, 128), F32)
    for _ in range(3):
        part = rest.astype(BF16)
        rest = rest - part.astype(F32)
        extra = extra + lax.dot_general(ST[1], part, NT, preferred_element_type=F32)
    for s in range(NY):
        H[s] = H[s] + GR[s]
        for i in range(HALF // 8):
            r = HALF * s + 8 * i
            H[s, i * CB + CB - 1] = H[s, i * CB + CB - 1] + extra[r : r + 8]

    def piece(h):
        return pl.ds(TX * h, TX)

    def down(t, h):
        return rcopy(
            H.at[lax.rem(y + NY // 2 - t, NY), piece(h)] if t == 0 or (t == 1 and h >= 2)
            else RF.at[t - 1, piece(h)],
            RF.at[t, piece(h)], f_send.at[t, h], f_recv.at[t, h], at_y(1),
        )

    def up(t, h):
        return rcopy(
            H.at[lax.rem(y + NY // 2 + t, NY), piece(h)] if t == 0 or (t == 1 and h < 2)
            else RB.at[t - 1, piece(h)],
            RB.at[t, piece(h)], k_send.at[t, h], k_recv.at[t, h], at_y(-1),
        )

    def forward(t):
        for h in range(NX):
            if t == 0:
                (down if h < 2 else up)(0, h).start()
                continue
            if t > 1 or h < 2:
                down(t - 1, h).wait_recv()
                RF[t - 1, piece(h)] = (
                    RF[t - 1, piece(h)] + H[lax.rem(y + NY // 2 - t, NY), piece(h)]
                )
            down(t, h).start()
            if t > 1 or h >= 2:
                up(t - 1, h).wait_recv()
                RB[t - 1, piece(h)] = (
                    RB[t - 1, piece(h)] + H[lax.rem(y + NY // 2 + t, NY), piece(h)]
                )
            up(t, h).start()

    forward(0)

    def reflat(ref, column):
        first_lane = lax.broadcasted_iota(jnp.int32, (8, 128), 1)

        def body(g, carry):
            tail = jnp.zeros((8, 128), F32)
            for k in range(16):
                off = CH * k
                first, sh = off // 128, off % 128
                v = column(g * 16 + k)
                if sh:
                    v = pltpu.roll(
                        jnp.concatenate([v, jnp.zeros((8, 128), F32)], axis=1), sh, axis=1
                    )
                    head = jnp.where(first_lane < sh, tail, v[:, :128])
                    v = jnp.concatenate([head, v[:, 128:]], axis=1)
                full = (sh + CH) // 128
                start = pl.multiple_of((g * GROUP + first) * 128, 128)
                ref[:, pl.ds(start, full * 128)] = v[0:ROWS, : full * 128].astype(BF16)
                if k < 15:
                    tail = v[:, full * 128 : full * 128 + 128]
            return carry

        lax.fori_loop(0, WIDTH // 16, body, 0)

    def out_column(w):
        normed = (PJ[w] - VEC[0:1]) * VEC[1:2]
        return X[w] + VEC[2:3] * normed + VEC[3:4]

    reflat(out_ref, out_column)
    forward(1)

    for cp in back:
        cp.wait()
    GD[1 : WIDTH + 1, ROWS, :] = jnp.where(y < NY - 1, BR[0].astype(F32), 0.0)
    GD[1 : WIDTH + 1, ROWS + 1, :] = jnp.where(y > 0, BR[1].astype(F32), 0.0)
    for b in range(CB):
        k = [dk_ref[t : t + 1, lanes(b)].astype(F32) for t in range(9)]

        def conv_t(q, carry):
            a = GD[pl.ds(q * 8, 10), :, lanes(b)]
            rows = [
                a[2:10] * k[3 * i] + a[1:9] * k[3 * i + 1] + a[0:8] * k[3 * i + 2]
                for i in range(3)
            ]
            d = pltpu.roll(rows[0], 7, axis=1) + rows[1] + pltpu.roll(rows[2], 1, axis=1)
            cols = pl.ds(q * 8, 8)
            PJ[cols, :, lanes(b)] = U[cols, :, lanes(b)] + jnp.where(
                X[cols, :, lanes(b)] > 0.0, d, 0.0
            )
            return carry

        lax.fori_loop(0, WIDTH // 8, conv_t, 0)
    forward(2)
    reflat(gin_ref, lambda w: PJ[w])
    forward(3)

    for h in range(NX):
        down(3, h).wait_recv()
        up(3, h).wait_recv()
        H[y, piece(h)] = H[y, piece(h)] + RF[3, piece(h)] + RB[3, piece(h)]
        d = lax.rem(h - xx + NX, NX)

        @pl.when(d != 0)
        def _():
            rcopy(
                H.at[y, piece(h)], VX.at[d - 1], x_send.at[d - 1], x_recv.at[d - 1],
                ((z * NX + h) * NC + c, y),
            ).start()

    v = H[y, pl.ds(pl.multiple_of(TX * xx, TX), TX)]
    for k in range(1, NX):
        cp = rcopy(VX.at[k - 1], VX.at[k - 1], x_send.at[k - 1], x_recv.at[k - 1], at_x(k))
        cp.wait_recv()
        v = v + VX[k - 1]
    GS[0, 0:TX] = v

    mine_i = (TX * z + NZ - 1) // NZ
    is_red = jnp.logical_and(mine_i < TX, (NZ * mine_i) // TX == z)

    def to_red(i):
        d = lax.rem(z - RED[i] + NZ, NZ)
        return rcopy(
            GS.at[0, i], VZ.at[d - 1], z_send.at[i], z_recv.at[d - 1], at_zz(RED[i])
        )

    for i in range(TX):

        @pl.when(z != RED[i])
        def _():
            to_red(i).start()

    @pl.when(is_red)
    def _():
        s = GS[0, mine_i]
        for d in range(1, NZ):
            rcopy(
                VZ.at[d - 1], VZ.at[d - 1], z_send.at[0], z_recv.at[d - 1],
                at_zz(lax.rem(z + d, NZ)),
            ).wait_recv()
            s = s + VZ[d - 1]
        C[c, TX * xx + mine_i] = s * (1.0 / BATCH)
        for d in range(1, NZ):
            tile = C.at[c, TX * xx + mine_i]
            rcopy(
                tile, tile, a_send.at[d - 1], a_recv.at[mine_i], at_zz(lax.rem(z + d, NZ))
            ).start()

    for i in range(TX):

        @pl.when(z != RED[i])
        def _():
            tile = C.at[c, TX * xx + i]
            rcopy(tile, tile, a_send.at[0], a_recv.at[i], at_zz(RED[i])).wait_recv()

    def part(core, x0):
        return C.at[core, pl.ds(pl.multiple_of(TX * x0, TX), TX)]

    for k in range(1, NX):
        rcopy(part(c, xx), part(c, xx), ax_send.at[k - 1], ax_recv.at[k - 1], at_x(k)).start()
    rcopy(part(c, xx), part(c, xx), ac_send.at[0], ac_recv.at[0], partner).start()
    for k in range(1, NX):
        x0 = lax.rem(xx - k + NX, NX)
        rcopy(part(c, x0), part(c, x0), ax_send.at[k - 1], ax_recv.at[k - 1], at_x(k)).wait_recv()
        rcopy(part(c, x0), part(c, x0), ac_send.at[k], ac_recv.at[k], partner).start()
    for k in range(NX):
        x0 = lax.rem(xx - k + NX, NX)
        cp = rcopy(part(1 - c, x0), part(1 - c, x0), ac_send.at[k], ac_recv.at[k], partner)
        cp.wait_recv()

    CM[...] = jnp.zeros_like(CM)
    for core in range(NC):
        for i in range(HALF // 8):
            for j in range(CB):
                r = core * HALF + 8 * i
                CM[r : r + 8, lanes(j)] = C[core, i * CB + j]
    for j in range(CB):
        t = CM[:, lanes(j)].T
        if j < CB - 1:
            gpw_ref[lanes(j), :] = t[:, :SHARE]
        else:
            cut = CH - 128 * j
            gpw_ref[128 * j : CH, :] = t[:cut, :SHARE]
            gdw_ref[...] = t[cut : cut + 9, :SHARE]
            gg_ref[...] = t[cut + 9 : cut + 10, :SHARE]
            gs_ref[...] = t[cut + 10 : cut + 11, :SHARE]

    for t in range(4):
        for h in range(NX):
            if t > 0 or h < 2:
                down(t, h).wait_send()
            if t > 0 or h >= 2:
                up(t, h).wait_send()
    for k in range(1, NX):
        rcopy(VX.at[k - 1], VX.at[k - 1], x_send.at[k - 1], x_recv.at[k - 1], at_x(k)).wait_send()
    for i in range(TX):

        @pl.when(z != RED[i])
        def _():
            to_red(i).wait_send()

    @pl.when(is_red)
    def _():
        for d in range(1, NZ):
            tile = C.at[c, TX * xx + mine_i]
            rcopy(
                tile, tile, a_send.at[d - 1], a_recv.at[mine_i], at_zz(lax.rem(z + d, NZ))
            ).wait_send()

    for k in range(1, NX):
        rcopy(part(c, xx), part(c, xx), ax_send.at[k - 1], ax_recv.at[k - 1], at_x(k)).wait_send()
    for k in range(NX):
        x0 = lax.rem(xx - k + NX, NX)
        rcopy(part(c, x0), part(c, x0), ac_send.at[k], ac_recv.at[k], partner).wait_send()


def local(inputs, upstream, labels, class_weights, depth_kernel, point_weight, gain, shift):
    vm = pl.BlockSpec(memory_space=pltpu.VMEM)
    dma = pltpu.SemaphoreType.DMA
    wide = (1, CP)

    def pad_row(row):
        return jnp.pad(row[None, :], ((0, 0), (0, CP - CH)))

    outs = pl.pallas_call(
        kernel,
        out_shape=(
            jax.ShapeDtypeStruct((ROWS, WIDTH * CH), BF16),
            jax.ShapeDtypeStruct((ROWS, WIDTH * CH), BF16),
            jax.ShapeDtypeStruct((CH, SHARE), F32),
            jax.ShapeDtypeStruct((9, SHARE), F32),
            jax.ShapeDtypeStruct((1, SHARE), F32),
            jax.ShapeDtypeStruct((1, SHARE), F32),
        ),
        in_specs=[vm, vm, vm, pl.BlockSpec(memory_space=pltpu.SMEM), vm, vm, vm, vm],
        out_specs=(vm,) * 6,
        scratch_shapes=[
            pltpu.VMEM((WIDTH, 8, CP), F32),
            pltpu.VMEM((WIDTH + 2, 8, CP), F32),
            pltpu.VMEM((WIDTH, 8, CP), F32),
            pltpu.VMEM((WIDTH, 8, CP), F32),
            pltpu.VMEM((PIX, CP), BF16),
            pltpu.VMEM((PIX, CP), BF16),
            pltpu.VMEM((WIDTH + 2, 8, CP), F32),
            pltpu.VMEM((CP, CP), BF16),
            pltpu.VMEM((2, NH, CP), BF16),
            pltpu.VMEM((NH, PIX), BF16),
            pltpu.VMEM((16, CP), F32),
            pltpu.VMEM((128, CP), F32),
            pltpu.VMEM((NY, TILES, 8, 128), F32),
            pltpu.VMEM((NY, TILES, 8, 128), F32),
            pltpu.VMEM((NY, TILES, 8, 128), F32),
            pltpu.VMEM((4, TILES, 8, 128), F32),
            pltpu.VMEM((4, TILES, 8, 128), F32),
            pltpu.VMEM((NX - 1, TX, 8, 128), F32),
            pltpu.VMEM((NZ - 1, 8, 128), F32),
            pltpu.VMEM((NC, TILES, 8, 128), F32),
            pltpu.VMEM((128, CP), F32),
            pltpu.VMEM((2, WIDTH, CP), BF16),
            pltpu.VMEM((2, WIDTH, CP), BF16),
            pltpu.VMEM((2, WIDTH, CP), BF16),
            pltpu.VMEM((2, WIDTH, CP), BF16),
            pltpu.VMEM((NY, 4, CP), F32),
            pltpu.VMEM((8, CP), F32),
            pltpu.VMEM((16, CP), F32),
            dma((2,)), dma((2,)), dma((2,)), dma((2,)),
            dma((NY - 1,)), dma((NY - 1,)), dma((2,)), dma((2,)),
            dma((4, NX)), dma((4, NX)), dma((4, NX)), dma((4, NX)),
            dma((NX - 1,)), dma((NX - 1,)), dma((TX,)), dma((NZ - 1,)),
            dma((NZ - 1,)), dma((TX,)), dma((NX - 1,)), dma((NX - 1,)),
            dma((NX,)), dma((NX,)),
        ],
        compiler_params=pltpu.CompilerParams(
            collective_id=0, has_side_effects=True, vmem_limit_bytes=48 * 1024 * 1024
        ),
    )(
        inputs.reshape(ROWS, WIDTH * CH),
        upstream.reshape(ROWS, WIDTH * CH),
        labels.reshape(ROWS, WIDTH),
        class_weights,
        jnp.pad(depth_kernel, ((0, 0), (0, CP - CH))),
        point_weight,
        pad_row(gain),
        pad_row(shift),
    )
    block_out, grad_in, gpw, gdw, gg, gs = outs
    return (
        block_out.reshape(1, ROWS, WIDTH * CH),
        grad_in.reshape(1, ROWS, WIDTH * CH),
        gpw,
        gdw,
        gg.reshape(SHARE),
        gs.reshape(SHARE),
    )


def solution(mesh):
    return jax.shard_map(
        local,
        mesh=mesh,
        in_specs=(
            P("dp", "slab", None),
            P("dp", "slab", None),
            P("dp", "slab", None),
            P(), P(), P(), P(), P(),
        ),
        out_specs=(
            P("dp", "slab", None),
            P("dp", "slab", None),
            P(None, "slab"),
            P(None, "slab"),
            P("slab"),
            P("slab"),
        ),
        check_vma=False,
    )
```

```python
import functools

import jax
import jax.numpy as jnp
from jax import lax
from jax.experimental import pallas as pl
from jax.experimental.pallas import tpu as pltpu
from jax.sharding import PartitionSpec as P

MESH = pl.DeviceIdType.MESH
F32 = jnp.float32
BF16 = jnp.bfloat16

CH = 728
CP = 768
CB = CP // 128
WIDTH = 48
ROWS = 6
PIX = WIDTH * 8
GROUP = 16 * CH // 128
NZ, NX, NC, NY = 16, 4, 2, 8
SHARE = CH // NY
HALF = 48
NH = NY * HALF
TILES = HALF // 8 * CB
TX = TILES // NX
RED = [NZ * i // TX for i in range(TX)]
COUNT = float(ROWS * WIDTH * NY)
BATCH = float(NZ * NX * NC)


def lanes(i):
    return slice(128 * i, 128 * (i + 1))


def kernel(
    x_hbm, u_hbm, lab_hbm, cw_hbm, dk_hbm, pw_hbm, gain_hbm, shift_hbm,
    out_ref, gin_ref, gpw_ref, gdw_ref, gg_ref, gs_ref,
    x_ref, u_ref, lab_ref, cw_ref, dk_ref, pw_ref, gain_ref, shift_ref, in_sem, DK,
    X, A, U, PJ, D, GP, GD, WP, ST, SEL, RR, RS, GS, GR, H, RF, RB, VX, VZ, C, CM,
    HS, HR, BS, BR, STAT, VEC, RRECV,
    h_send, h_recv, b_send, b_recv, s_send, s_recv, g_send, g_recv,
    f_send, f_recv, k_send, k_recv, x_send, x_recv, z_send, z_recv,
    a_send, a_recv, ax_send, ax_recv, ac_send, ac_recv,
):
    dp = lax.axis_index("dp")
    y = lax.axis_index("slab")
    c = lax.rem(dp, NC)
    xx = lax.rem(dp // NC, NX)
    z = dp // (NC * NX)

    def at_y(k):
        return (dp, lax.rem(y + (k % NY), NY))

    def at_x(k):
        return ((z * NX + lax.rem(xx + (k % NX), NX)) * NC + c, y)

    def at_zz(zz):
        return ((zz * NX + xx) * NC + c, y)

    partner = ((z * NX + xx) * NC + (1 - c), y)

    def rcopy(src, dst, ss, rs, dev):
        return pltpu.make_async_remote_copy(
            src_ref=src, dst_ref=dst, send_sem=ss, recv_sem=rs,
            device_id=dev, device_id_type=MESH,
        )

    loads = [
        pltpu.make_async_copy(src, dst, in_sem.at[i])
        for i, (src, dst) in enumerate((
            (x_hbm, x_ref), (u_hbm, u_ref), (lab_hbm, lab_ref), (cw_hbm, cw_ref),
            (dk_hbm, dk_ref), (pw_hbm, pw_ref), (gain_hbm, gain_ref), (shift_hbm, shift_ref),
        ))
    ]
    for cp in loads:
        cp.start()
    barrier = pltpu.get_barrier_semaphore()
    peers = [at_y(k) for k in range(1, NY)]
    peers += [at_x(k) for k in range(1, NX)]
    peers += [at_zz(lax.rem(z + k, NZ)) for k in range(1, NZ)]
    peers += [partner]
    for peer in peers:
        pl.semaphore_signal(barrier, inc=1, device_id=peer, device_id_type=MESH)

    lane_ok = lax.broadcasted_iota(jnp.int32, (ROWS, CP), 1) < CH

    def unflat(ref, base, k):
        off = CH * k
        first, sh = off // 128, off % 128
        nv = 6 if sh + CH <= CP else 7
        v = ref[:, pl.ds(pl.multiple_of(base + first * 128, 128), nv * 128)].astype(F32)
        if sh:
            v = pltpu.roll(v, nv * 128 - sh, axis=1)
        return jnp.where(lane_ok, v[:, :CP], 0.0)

    X[...] = jnp.zeros_like(X)
    U[...] = jnp.zeros_like(U)
    WP[...] = jnp.zeros_like(WP)
    DK[...] = jnp.zeros_like(DK)
    loads[0].wait()

    def load_x(g, carry):
        for k in range(16):
            X[g * 16 + k, 0:ROWS, :] = unflat(x_ref, g * GROUP * 128, k)
        return carry

    lax.fori_loop(0, WIDTH // 16, load_x, 0)
    for side, row in ((0, 0), (1, ROWS - 1)):
        HS[side] = X[:, row, :].astype(BF16)

    for cp in loads[1:]:
        cp.wait()
    lab = jnp.concatenate([lab_ref[r] for r in range(ROWS)], axis=0)
    DK[0:9, 0:CH] = dk_ref[...].astype(F32)
    wt = jnp.where(
        lab == 0, cw_ref[0], jnp.where(lab == 1, cw_ref[1], jnp.where(lab == 2, cw_ref[2], 0.0))
    )
    for w in range(WIDTH):
        U[w, 0:ROWS, :] = unflat(u_ref, (w // 16) * GROUP * 128, w % 16) * wt[:, w : w + 1]

    pl.semaphore_wait(barrier, len(peers))

    halo = [
        rcopy(HS.at[0], HR.at[0], h_send.at[0], h_recv.at[0], at_y(-1)),
        rcopy(HS.at[1], HR.at[1], h_send.at[1], h_recv.at[1], at_y(1)),
    ]
    for cp in halo:
        cp.start()

    WP[0:CH, 0:CH] = pw_ref[...]
    row = lax.broadcasted_iota(jnp.int32, (NH, 128), 0)
    slab_of = jnp.zeros_like(row)
    for k in range(1, NY):
        slab_of = slab_of + jnp.where(row >= HALF * k, 1, 0)
    inner = row - HALF * slab_of
    lane = lax.broadcasted_iota(jnp.int32, (NH, 128), 1)
    for h in range(2):
        core = (1 - c) if h == 0 else c
        j = inner + HALF * core
        target = jnp.where(j < SHARE, SHARE * slab_of + j, -1)
        for b in range(CB):
            ST[h, :, lanes(b)] = jnp.where(lane + 128 * b == target, 1.0, 0.0).astype(BF16)

    for cp in halo:
        cp.wait()
    below = jnp.where(y < NY - 1, HR[0].astype(F32), 0.0)
    above = jnp.where(y > 0, HR[1].astype(F32), 0.0)
    X[:, ROWS, :] = below
    X[:, ROWS + 1, :] = above
    A[0] = jnp.zeros((8, CP), F32)
    A[WIDTH + 1] = jnp.zeros((8, CP), F32)
    A[1 : WIDTH + 1] = jnp.maximum(X[...], 0.0)

    own = lax.broadcasted_iota(jnp.int32, (8, 8, 128), 1) < ROWS
    own2 = lax.broadcasted_iota(jnp.int32, (8, 8, 128), 1) < ROWS

    for b in range(CB):
        k = [DK[t : t + 1, lanes(b)] for t in range(9)]

        def conv(q, carry):
            a = A[pl.ds(q * 8, 10), :, lanes(b)]
            rows = [
                a[0:8] * k[3 * i] + a[1:9] * k[3 * i + 1] + a[2:10] * k[3 * i + 2]
                for i in range(3)
            ]
            d = pltpu.roll(rows[0], 1, axis=1) + rows[1] + pltpu.roll(rows[2], 7, axis=1)
            d = jnp.where(own, d, 0.0)
            D[pl.ds(pl.multiple_of(q * 64, 64), 64), lanes(b)] = d.reshape(64, 128).astype(BF16)
            return carry

        lax.fori_loop(0, WIDTH // 8, conv, 0)

    for nb in range(3):
        cols = slice(256 * nb, 256 * (nb + 1))
        PJ[:, :, cols] = jnp.dot(
            D[...], WP[:, cols], preferred_element_type=F32
        ).reshape(WIDTH, 8, 256)

    n_local = float(ROWS * WIDTH)
    for b in range(CB):
        s = jnp.zeros((8, 128), F32)
        g = jnp.zeros((8, 128), F32)
        for q in range(WIDTH // 8):
            s = s + jnp.sum(PJ[8 * q : 8 * q + 8, :, lanes(b)], axis=0)
            g = g + jnp.sum(U[8 * q : 8 * q + 8, :, lanes(b)], axis=0)
        s = jnp.sum(s, axis=0, keepdims=True)
        g = jnp.sum(g, axis=0, keepdims=True)
        mu = s * (1.0 / n_local)
        m2 = jnp.zeros((8, 128), F32)
        cr = jnp.zeros((8, 128), F32)
        for q in range(WIDTH // 8):
            dev = jnp.where(own2, PJ[8 * q : 8 * q + 8, :, lanes(b)] - mu, 0.0)
            m2 = m2 + jnp.sum(dev * dev, axis=0)
            cr = cr + jnp.sum(dev * U[8 * q : 8 * q + 8, :, lanes(b)], axis=0)
        m2 = jnp.sum(m2, axis=0, keepdims=True)
        cr = jnp.sum(cr, axis=0, keepdims=True)
        STAT[y, :, lanes(b)] = jnp.concatenate([s, g, m2, cr], axis=0)
    stat = []
    for k in range(1, NY):
        cp = rcopy(STAT.at[y], STAT.at[y], s_send.at[k - 1], s_recv.at[k - 1], at_y(k))
        cp.start()
        stat.append(cp)
    for cp in stat:
        cp.wait()

    total = STAT[0, 0:2, :]
    for i in range(1, NY):
        total = total + STAT[i, 0:2, :]
    center = total[0:1] * (1.0 / COUNT)
    shift_part = total[1:2]
    square = jnp.zeros((1, CP), F32)
    cross = jnp.zeros((1, CP), F32)
    for i in range(NY):
        off = STAT[i, 0:1, :] * (1.0 / n_local) - center
        square = square + STAT[i, 2:3, :] + n_local * off * off
        cross = cross + STAT[i, 3:4, :] + off * STAT[i, 1:2, :]
    inverse = lax.rsqrt(square * (1.0 / COUNT) + 1e-05)
    gain_part = cross * inverse
    mine = STAT[y]
    off = mine[0:1] * (1.0 / n_local) - center
    gain_local = (mine[3:4] + off * mine[1:2]) * inverse
    shift_local = mine[1:2]
    pad = jnp.zeros((1, CP - CH), F32)
    gain = jnp.concatenate([gain_ref[...].reshape(1, CH), pad], axis=1)
    VEC[0:1] = center
    VEC[1:2] = inverse
    VEC[2:3] = gain
    VEC[3:4] = jnp.concatenate([shift_ref[...].reshape(1, CH), pad], axis=1)
    VEC[4:5] = gain * inverse
    VEC[5:6] = shift_part * (1.0 / COUNT)
    VEC[6:7] = gain_part * (1.0 / COUNT)

    for b in range(CB):
        v = [VEC[i : i + 1, lanes(b)] for i in range(7)]

        def proj(q, carry):
            rows = pl.ds(q * 8, 8)
            normed = (PJ[rows, :, lanes(b)] - v[0]) * v[1]
            gp = v[4] * (U[rows, :, lanes(b)] - v[5] - normed * v[6])
            gp = jnp.where(own, gp, 0.0)
            GP[pl.ds(pl.multiple_of(q * 64, 64), 64), lanes(b)] = gp.reshape(64, 128).astype(BF16)
            return carry

        lax.fori_loop(0, WIDTH // 8, proj, 0)

    NT = (((1,), (1,)), ((), ()))

    def weight_half(h, dst):
        SEL[...] = lax.dot_general(
            ST[h], GP[...], NT, preferred_element_type=F32
        ).astype(BF16)
        for nb in range(3):
            part = jnp.dot(
                SEL[...], D[:, 256 * nb : 256 * nb + 256], preferred_element_type=F32
            )
            for s in range(NY):
                for i in range(HALF // 8):
                    for j in range(2):
                        r = HALF * s + 8 * i
                        dst[s, i * CB + 2 * nb + j] = part[r : r + 8, lanes(j)]

    weight_half(0, GS)
    g_copy = rcopy(GS, GR, g_send.at[0], g_recv.at[0], partner)
    g_copy.start()

    GD[0] = jnp.zeros((8, CP), F32)
    GD[WIDTH + 1] = jnp.zeros((8, CP), F32)
    for nb in range(3):
        rows = slice(256 * nb, 256 * (nb + 1))
        gd = lax.dot_general(GP[...], WP[rows, :], NT, preferred_element_type=F32)
        GD[1 : WIDTH + 1, :, rows] = gd.astype(BF16).astype(F32).reshape(WIDTH, 8, 256)
    BS[0] = GD[1 : WIDTH + 1, 0, :].astype(BF16)
    BS[1] = GD[1 : WIDTH + 1, ROWS - 1, :].astype(BF16)
    back = [
        rcopy(BS.at[0], BR.at[0], b_send.at[0], b_recv.at[0], at_y(-1)),
        rcopy(BS.at[1], BR.at[1], b_send.at[1], b_recv.at[1], at_y(1)),
    ]
    for cp in back:
        cp.start()

    RR[...] = jnp.zeros_like(RR)
    for b in range(CB):

        def tap(q, acc):
            a = A[pl.ds(q * 8, 10), :, lanes(b)]
            gd = GD[pl.ds(q * 8 + 1, 8), :, lanes(b)]
            shifted = [pltpu.roll(gd, 7, axis=1), gd, pltpu.roll(gd, 1, axis=1)]
            return tuple(
                acc[3 * i + j] + jnp.sum(a[j : j + 8] * shifted[i], axis=0)
                for i in range(3)
                for j in range(3)
            )

        acc = lax.fori_loop(
            0, WIDTH // 8, tap, tuple(jnp.zeros((8, 128), F32) for _ in range(9))
        )
        for t in range(9):
            RR[t : t + 1, lanes(b)] = jnp.sum(acc[t], axis=0, keepdims=True)
    RR[9:10] = gain_local
    RR[10:11] = shift_local
    r_copy = rcopy(RR, RRECV, g_send.at[1], g_recv.at[1], partner)
    r_copy.start()

    weight_half(1, H)
    RS[...] = jnp.zeros_like(RS)
    g_copy.wait()
    r_copy.wait()
    RS[CH - 640 : CH - 640 + 16] = RR[...] + RRECV[...]
    rest = RS[...]
    extra = jnp.zeros((NH, 128), F32)
    for _ in range(3):
        part = rest.astype(BF16)
        rest = rest - part.astype(F32)
        extra = extra + lax.dot_general(ST[1], part, NT, preferred_element_type=F32)
    for s in range(NY):
        H[s] = H[s] + GR[s]
        for i in range(HALF // 8):
            r = HALF * s + 8 * i
            H[s, i * CB + CB - 1] = H[s, i * CB + CB - 1] + extra[r : r + 8]

    def piece(h):
        return pl.ds(TX * h, TX)

    def down(t, h):
        return rcopy(
            H.at[lax.rem(y + NY // 2 - t, NY), piece(h)] if t == 0 or (t == 1 and h >= 2)
            else RF.at[t - 1, piece(h)],
            RF.at[t, piece(h)], f_send.at[t, h], f_recv.at[t, h], at_y(1),
        )

    def up(t, h):
        return rcopy(
            H.at[lax.rem(y + NY // 2 + t, NY), piece(h)] if t == 0 or (t == 1 and h < 2)
            else RB.at[t - 1, piece(h)],
            RB.at[t, piece(h)], k_send.at[t, h], k_recv.at[t, h], at_y(-1),
        )

    def forward(t):
        for h in range(NX):
            if t == 0:
                (down if h < 2 else up)(0, h).start()
                continue
            if t > 1 or h < 2:
                down(t - 1, h).wait_recv()
                RF[t - 1, piece(h)] = (
                    RF[t - 1, piece(h)] + H[lax.rem(y + NY // 2 - t, NY), piece(h)]
                )
            down(t, h).start()
            if t > 1 or h >= 2:
                up(t - 1, h).wait_recv()
                RB[t - 1, piece(h)] = (
                    RB[t - 1, piece(h)] + H[lax.rem(y + NY // 2 + t, NY), piece(h)]
                )
            up(t, h).start()

    forward(0)

    def reflat(ref, column):
        first_lane = lax.broadcasted_iota(jnp.int32, (8, 128), 1)

        def body(g, carry):
            tail = jnp.zeros((8, 128), F32)
            for k in range(16):
                off = CH * k
                first, sh = off // 128, off % 128
                v = column(g * 16 + k)
                if sh:
                    v = pltpu.roll(
                        jnp.concatenate([v, jnp.zeros((8, 128), F32)], axis=1), sh, axis=1
                    )
                    head = jnp.where(first_lane < sh, tail, v[:, :128])
                    v = jnp.concatenate([head, v[:, 128:]], axis=1)
                full = (sh + CH) // 128
                start = pl.multiple_of((g * GROUP + first) * 128, 128)
                ref[:, pl.ds(start, full * 128)] = v[0:ROWS, : full * 128].astype(BF16)
                if k < 15:
                    tail = v[:, full * 128 : full * 128 + 128]
            return carry

        lax.fori_loop(0, WIDTH // 16, body, 0)

    def out_column(w):
        normed = (PJ[w] - VEC[0:1]) * VEC[1:2]
        return X[w] + VEC[2:3] * normed + VEC[3:4]

    reflat(out_ref, out_column)
    forward(1)

    for cp in back:
        cp.wait()
    GD[1 : WIDTH + 1, ROWS, :] = jnp.where(y < NY - 1, BR[0].astype(F32), 0.0)
    GD[1 : WIDTH + 1, ROWS + 1, :] = jnp.where(y > 0, BR[1].astype(F32), 0.0)
    for b in range(CB):
        k = [DK[t : t + 1, lanes(b)] for t in range(9)]

        def conv_t(q, carry):
            a = GD[pl.ds(q * 8, 10), :, lanes(b)]
            rows = [
                a[2:10] * k[3 * i] + a[1:9] * k[3 * i + 1] + a[0:8] * k[3 * i + 2]
                for i in range(3)
            ]
            d = pltpu.roll(rows[0], 7, axis=1) + rows[1] + pltpu.roll(rows[2], 1, axis=1)
            cols = pl.ds(q * 8, 8)
            PJ[cols, :, lanes(b)] = U[cols, :, lanes(b)] + jnp.where(
                X[cols, :, lanes(b)] > 0.0, d, 0.0
            )
            return carry

        lax.fori_loop(0, WIDTH // 8, conv_t, 0)
    forward(2)
    reflat(gin_ref, lambda w: PJ[w])
    forward(3)

    for h in range(NX):
        down(3, h).wait_recv()
        up(3, h).wait_recv()
        H[y, piece(h)] = H[y, piece(h)] + RF[3, piece(h)] + RB[3, piece(h)]
        d = lax.rem(h - xx + NX, NX)

        @pl.when(d != 0)
        def _():
            rcopy(
                H.at[y, piece(h)], VX.at[d - 1], x_send.at[d - 1], x_recv.at[d - 1],
                ((z * NX + h) * NC + c, y),
            ).start()

    v = H[y, pl.ds(pl.multiple_of(TX * xx, TX), TX)]
    for k in range(1, NX):
        cp = rcopy(VX.at[k - 1], VX.at[k - 1], x_send.at[k - 1], x_recv.at[k - 1], at_x(k))
        cp.wait_recv()
        v = v + VX[k - 1]
    GS[0, 0:TX] = v

    mine_i = (TX * z + NZ - 1) // NZ
    is_red = jnp.logical_and(mine_i < TX, (NZ * mine_i) // TX == z)

    def to_red(i):
        d = lax.rem(z - RED[i] + NZ, NZ)
        return rcopy(
            GS.at[0, i], VZ.at[d - 1], z_send.at[i], z_recv.at[d - 1], at_zz(RED[i])
        )

    for i in range(TX):

        @pl.when(z != RED[i])
        def _():
            to_red(i).start()

    @pl.when(is_red)
    def _():
        s = GS[0, mine_i]
        for d in range(1, NZ):
            rcopy(
                VZ.at[d - 1], VZ.at[d - 1], z_send.at[0], z_recv.at[d - 1],
                at_zz(lax.rem(z + d, NZ)),
            ).wait_recv()
            s = s + VZ[d - 1]
        C[c, TX * xx + mine_i] = s * (1.0 / BATCH)
        for d in range(1, NZ):
            tile = C.at[c, TX * xx + mine_i]
            rcopy(
                tile, tile, a_send.at[d - 1], a_recv.at[mine_i], at_zz(lax.rem(z + d, NZ))
            ).start()

    for i in range(TX):

        @pl.when(z != RED[i])
        def _():
            tile = C.at[c, TX * xx + i]
            rcopy(tile, tile, a_send.at[0], a_recv.at[i], at_zz(RED[i])).wait_recv()

    def part(core, x0):
        return C.at[core, pl.ds(pl.multiple_of(TX * x0, TX), TX)]

    for k in range(1, NX):
        rcopy(part(c, xx), part(c, xx), ax_send.at[k - 1], ax_recv.at[k - 1], at_x(k)).start()
    rcopy(part(c, xx), part(c, xx), ac_send.at[0], ac_recv.at[0], partner).start()
    for k in range(1, NX):
        x0 = lax.rem(xx - k + NX, NX)
        rcopy(part(c, x0), part(c, x0), ax_send.at[k - 1], ax_recv.at[k - 1], at_x(k)).wait_recv()
        rcopy(part(c, x0), part(c, x0), ac_send.at[k], ac_recv.at[k], partner).start()
    for k in range(NX):
        x0 = lax.rem(xx - k + NX, NX)
        cp = rcopy(part(1 - c, x0), part(1 - c, x0), ac_send.at[k], ac_recv.at[k], partner)
        cp.wait_recv()

    CM[...] = jnp.zeros_like(CM)
    for core in range(NC):
        for i in range(HALF // 8):
            for j in range(CB):
                r = core * HALF + 8 * i
                CM[r : r + 8, lanes(j)] = C[core, i * CB + j]
    gpw_ref[...] = CM[0:SHARE, 0:CH]
    cut = CH - 128 * (CB - 1)
    t = CM[:, lanes(CB - 1)].T
    gdw_ref[...] = t[cut : cut + 9, :SHARE]
    gg_ref[...] = t[cut + 9 : cut + 10, :SHARE]
    gs_ref[...] = t[cut + 10 : cut + 11, :SHARE]

    for t in range(4):
        for h in range(NX):
            if t > 0 or h < 2:
                down(t, h).wait_send()
            if t > 0 or h >= 2:
                up(t, h).wait_send()
    for k in range(1, NX):
        rcopy(VX.at[k - 1], VX.at[k - 1], x_send.at[k - 1], x_recv.at[k - 1], at_x(k)).wait_send()
    for i in range(TX):

        @pl.when(z != RED[i])
        def _():
            to_red(i).wait_send()

    @pl.when(is_red)
    def _():
        for d in range(1, NZ):
            tile = C.at[c, TX * xx + mine_i]
            rcopy(
                tile, tile, a_send.at[d - 1], a_recv.at[mine_i], at_zz(lax.rem(z + d, NZ))
            ).wait_send()

    for k in range(1, NX):
        rcopy(part(c, xx), part(c, xx), ax_send.at[k - 1], ax_recv.at[k - 1], at_x(k)).wait_send()
    for k in range(NX):
        x0 = lax.rem(xx - k + NX, NX)
        rcopy(part(c, x0), part(c, x0), ac_send.at[k], ac_recv.at[k], partner).wait_send()


def store(*refs):
    sem = refs[12]
    copies = [pltpu.make_async_copy(refs[i], refs[6 + i], sem.at[i]) for i in range(6)]
    for cp in copies:
        cp.start()
    for cp in copies:
        cp.wait()


def local(inputs, upstream, labels, class_weights, depth_kernel, point_weight, gain, shift):
    vm = pl.BlockSpec(memory_space=pltpu.VMEM)
    dma = pltpu.SemaphoreType.DMA
    hbm = pl.BlockSpec(memory_space=pltpu.HBM)
    shapes = (
            jax.ShapeDtypeStruct((ROWS, WIDTH * CH), BF16),
            jax.ShapeDtypeStruct((ROWS, WIDTH * CH), BF16),
            jax.ShapeDtypeStruct((SHARE, CH), F32),
            jax.ShapeDtypeStruct((9, SHARE), F32),
            jax.ShapeDtypeStruct((1, SHARE), F32),
            jax.ShapeDtypeStruct((1, SHARE), F32),
    )
    outs = pl.pallas_call(
        kernel,
        out_shape=shapes,
        in_specs=[hbm] * 8,
        out_specs=(vm,) * 6,
        scratch_shapes=[
            pltpu.VMEM((ROWS, WIDTH * CH), BF16),
            pltpu.VMEM((ROWS, WIDTH * CH), BF16),
            pltpu.VMEM((ROWS, 1, WIDTH), jnp.int32),
            pltpu.SMEM((3,), F32),
            pltpu.VMEM((9, CH), BF16),
            pltpu.VMEM((CH, CH), BF16),
            pltpu.VMEM((CH,), F32),
            pltpu.VMEM((CH,), F32),
            dma((8,)),
            pltpu.VMEM((16, CP), F32),
            pltpu.VMEM((WIDTH, 8, CP), F32),
            pltpu.VMEM((WIDTH + 2, 8, CP), F32),
            pltpu.VMEM((WIDTH, 8, CP), F32),
            pltpu.VMEM((WIDTH, 8, CP), F32),
            pltpu.VMEM((PIX, CP), BF16),
            pltpu.VMEM((PIX, CP), BF16),
            pltpu.VMEM((WIDTH + 2, 8, CP), F32),
            pltpu.VMEM((CP, CP), BF16),
            pltpu.VMEM((2, NH, CP), BF16),
            pltpu.VMEM((NH, PIX), BF16),
            pltpu.VMEM((16, CP), F32),
            pltpu.VMEM((128, CP), F32),
            pltpu.VMEM((NY, TILES, 8, 128), F32),
            pltpu.VMEM((NY, TILES, 8, 128), F32),
            pltpu.VMEM((NY, TILES, 8, 128), F32),
            pltpu.VMEM((4, TILES, 8, 128), F32),
            pltpu.VMEM((4, TILES, 8, 128), F32),
            pltpu.VMEM((NX - 1, TX, 8, 128), F32),
            pltpu.VMEM((NZ - 1, 8, 128), F32),
            pltpu.VMEM((NC, TILES, 8, 128), F32),
            pltpu.VMEM((128, CP), F32),
            pltpu.VMEM((2, WIDTH, CP), BF16),
            pltpu.VMEM((2, WIDTH, CP), BF16),
            pltpu.VMEM((2, WIDTH, CP), BF16),
            pltpu.VMEM((2, WIDTH, CP), BF16),
            pltpu.VMEM((NY, 4, CP), F32),
            pltpu.VMEM((8, CP), F32),
            pltpu.VMEM((16, CP), F32),
            dma((2,)), dma((2,)), dma((2,)), dma((2,)),
            dma((NY - 1,)), dma((NY - 1,)), dma((2,)), dma((2,)),
            dma((4, NX)), dma((4, NX)), dma((4, NX)), dma((4, NX)),
            dma((NX - 1,)), dma((NX - 1,)), dma((TX,)), dma((NZ - 1,)),
            dma((NZ - 1,)), dma((TX,)), dma((NX - 1,)), dma((NX - 1,)),
            dma((NX,)), dma((NX,)),
        ],
        compiler_params=pltpu.CompilerParams(
            collective_id=0, has_side_effects=True, vmem_limit_bytes=48 * 1024 * 1024
        ),
    )(
        *(
            pltpu.with_memory_space_constraint(a, pltpu.HBM)
            for a in (
                inputs.reshape(ROWS, WIDTH * CH),
                upstream.reshape(ROWS, WIDTH * CH),
                labels.reshape(ROWS, 1, WIDTH),
                class_weights,
                depth_kernel,
                point_weight,
                gain,
                shift,
            )
        )
    )
    outs = pl.pallas_call(
        store,
        out_shape=shapes,
        in_specs=[vm] * 6,
        out_specs=(hbm,) * 6,
        scratch_shapes=[dma((6,))],
    )(*(pltpu.with_memory_space_constraint(a, pltpu.VMEM) for a in outs))
    block_out, grad_in, gpw, gdw, gg, gs = outs
    return (
        block_out.reshape(1, ROWS, WIDTH * CH),
        grad_in.reshape(1, ROWS, WIDTH * CH),
        gpw.T,
        gdw,
        gg.reshape(SHARE),
        gs.reshape(SHARE),
    )


def solution(mesh):
    return jax.shard_map(
        local,
        mesh=mesh,
        in_specs=(
            P("dp", "slab", None),
            P("dp", "slab", None),
            P("dp", "slab", None),
            P(), P(), P(), P(), P(),
        ),
        out_specs=(
            P("dp", "slab", None),
            P("dp", "slab", None),
            P(None, "slab"),
            P(None, "slab"),
            P("slab"),
            P("slab"),
        ),
        check_vma=False,
    )
```
